32 devices in a mesh: row: 4 (over z), col: 8 (over y, x, core).
Axes of the slice: x: 2, y: 2, z: 4, core: 2. Of those that a mesh axis runs over, the one named last changes fastest.
Arguments:
- grad_terms: bfloat16 [8, 2, 4096, 10240], P('col', None, 'row'), may hold values from -25 to 25, as said below
- row_moment: float32 [2, 4096], P(None, 'row'), may hold values from 0.01 to 3
- col_moment: float32 [2, 10240], P(None, 'col'), may hold values from 0.01 to 1
Outputs:
- update: float32 [2, 4096, 10240], P(None, 'row', 'col')
- new_rows: float32 [2, 4096], P(None, 'row')
- new_cols: float32 [2, 10240], P(None, 'col')
The draws below stay inside these ranges and needn't reach their ends.
Inputs may be any that keep to these rules, and one draw needn't show every extreme that they name: `grad_terms`: partial gradient terms of the 8 batch shards.
All inputs are finite; a program needn't handle non-finite values.
Results may differ from the reference program's by a relative error of at most 0.0003.
Values sent between devices are 32-bit elements; how exact they have to be, the bound alone decides.
A program may use at most 256 MiB of HBM per device.

```python
import math
import jax
import jax.numpy as jnp
from jax import lax

D = 4096
FF = 10240
MATS = 2
SOURCES = 8


def draw_grad_terms(key, part):
    subkeys = jax.random.split(key, 4)
    full_shape = (SOURCES, MATS, D, FF)
    chosen = jax.random.randint(subkeys[0], (), 0, MATS)
    factor = jnp.where(jnp.arange(MATS) == chosen, 1.0, 0.05).astype(jnp.float32)
    row_scale = jnp.exp(jax.random.uniform(subkeys[1], (MATS, D, 1), jnp.float32, jnp.log(0.3), jnp.log(3.0)))
    col_scale = jnp.exp(jax.random.uniform(subkeys[2], (MATS, 1, FF), jnp.float32, jnp.log(0.3), jnp.log(3.0)))
    base_values = 0.25 * jax.random.truncated_normal(subkeys[3], -4.0, 4.0, full_shape, jnp.float32)
    values = base_values * row_scale[None] * col_scale[None] * factor[None, :, None, None]
    return values.astype(jnp.bfloat16)


def draw_row_moment(key, part):
    subkeys = jax.random.split(jax.random.fold_in(key, 17), 1)
    position = jnp.arange(D, dtype=jnp.float32)[None, :] / jnp.float32(D - 1)
    rough = jnp.exp(jax.random.uniform(subkeys[0], (MATS, D), jnp.float32, jnp.log(0.02), jnp.log(0.2)))
    rising = jnp.exp(position * jnp.log(10.0))
    return (rough * rising).astype(jnp.float32)


def levels(rng, extent, pieces, smallest, top_value):
    def one(dim, shards_of):
        draws = jax.random.uniform(jax.random.fold_in(jax.random.fold_in(rng, 6), dim), (shards_of,), jnp.float32, smallest / len(pieces), top_value / len(pieces))
        return jnp.repeat(jnp.exp(draws), extent[dim] // shards_of).reshape((-1,) + (1,) * (len(extent) - dim - 1))

    gain = one(*pieces[0])
    for cut in pieces[1:]:
        gain = gain * one(*cut)
    return gain


def setup_inputs(seed: int = 0) -> dict:
    keys = jax.random.split(jax.random.key(seed), 4)
    grad_terms = draw_grad_terms(jax.random.fold_in(keys[3], 71), 0)
    row_moment = draw_row_moment(jax.random.fold_in(keys[3], 71), 0)
    col_moment = jnp.clip(jnp.exp(math.log(1.0) - 4.6051702 * jax.random.uniform(keys[2], (MATS, FF), jnp.float32) ** levels(keys[2], (MATS, FF), ((1, 8),), -0.2, 0.2)), 0.01, 1.0)
    return dict(grad_terms=grad_terms, row_moment=row_moment, col_moment=col_moment)


second_decay = 1.0 - 100.0 ** (-0.8)
tiny_square = 1e-30

def reference(grad_terms, row_moment, col_moment):

    def accumulate(source, running):
        return running + grad_terms[source].astype(jnp.float32)
    gradient = lax.fori_loop(0, grad_terms.shape[0], accumulate, jnp.zeros(grad_terms.shape[1:], jnp.float32))
    squares = gradient * gradient + tiny_square
    new_rows = second_decay * row_moment + (1.0 - second_decay) * lax.optimization_barrier(jnp.sum(squares, axis=2)) / FF
    new_cols = second_decay * col_moment + (1.0 - second_decay) * lax.optimization_barrier(jnp.sum(squares, axis=1)) / D
    row_level = lax.optimization_barrier(jnp.sum(new_rows, axis=1)) / D
    estimate = new_rows[:, :, None] * new_cols[:, None, :] / row_level[:, None, None]
    raw_update = gradient / jnp.sqrt(estimate)
    clip_scale = jnp.maximum(1.0, jnp.sqrt(lax.optimization_barrier(jnp.sum(raw_update * raw_update, axis=(1, 2))) / (D * FF)))
    update = raw_update / clip_scale[:, None, None]
    return (update, new_rows, new_cols)
```

```python
import jax
import jax.numpy as jnp
from jax import lax
from jax.sharding import PartitionSpec as P

second_decay = 1.0 - 100.0 ** (-0.8)
tiny_square = 1e-30
PIECES = 2


def scatter_piece(grad_terms, matrix, first, count, order, n, send_at, keep_at):
    width = grad_terms.shape[3] // n

    def own(r, me):
        start = jnp.bitwise_xor(me, r) * width
        block = lax.dynamic_slice(grad_terms, (0, matrix, first, start), (1, 1, count, width))
        return block.reshape(count, width).astype(jnp.float32)

    held = {r: own(r, send_at if r & order[0] else keep_at) for r in range(n)}
    for step, bit in enumerate(order):
        pairs = [(d, d ^ bit) for d in range(n)]
        sent = [r for r in held if r & bit]
        if step == 0:
            send_at, *tied = lax.optimization_barrier((send_at, *[held[r] for r in sent]))
            held.update(zip(sent, tied))
        arrived = {r ^ bit: lax.ppermute(held[r], "col", pairs) for r in sent}
        held = {r: held[r] + arrived[r] for r in held if not r & bit}
        if step == 0:
            kept = list(held)
            keep_at, *tied = lax.optimization_barrier((keep_at, *[held[r] for r in kept]))
            held = dict(zip(kept, tied))
    return held[0], send_at, keep_at


def on_device(n, grad_terms, row_moment, col_moment):
    mats, rows, columns = grad_terms.shape[1:]
    ff = columns
    d = rows * lax.axis_size("row")
    bits = [1 << b for b in range(n.bit_length() - 1)]
    orders = (bits, bits[:1] + bits[:0:-1])
    step = rows // (2 * PIECES)
    matrices, kept_at = [], []
    send_at = keep_at = lax.axis_index("col")
    for m in range(mats):
        pieces = []
        for p in range(2 * PIECES):
            if len(kept_at) >= 2:
                send_at = jnp.maximum(send_at, kept_at[-2])
            piece, send_at, keep_at = scatter_piece(
                grad_terms, m, p * step, step, orders[p % 2], n, send_at, keep_at
            )
            kept_at.append(keep_at)
            pieces.append(piece)
        matrices.append(jnp.concatenate(pieces, axis=0))
    gradient = jnp.stack(matrices)
    squares = gradient * gradient + tiny_square
    row_full = lax.psum(jnp.sum(squares, axis=2), "col")
    col_full = lax.psum(jnp.sum(squares, axis=1), "row")
    new_rows = second_decay * row_moment + (1.0 - second_decay) * row_full / ff
    new_cols = second_decay * col_moment + (1.0 - second_decay) * col_full / d
    row_gain = lax.rsqrt(new_rows)
    col_gain = lax.rsqrt(new_cols)
    scaled = gradient * row_gain[:, :, None] * col_gain[:, None, :]
    square_part = jnp.sum(scaled * scaled, axis=(1, 2))
    both = lax.psum(jnp.stack([square_part, jnp.sum(new_rows, axis=1) / n]), ("row", "col"))
    row_level = both[1] / d
    clip_scale = jnp.maximum(1.0, jnp.sqrt(both[0] * row_level / (d * ff)))
    update = scaled * (jnp.sqrt(row_level) / clip_scale)[:, None, None]
    return (update, new_rows, new_cols)


def solution(mesh):
    n = mesh.shape["col"]
    placed = (P("col", None, "row", None), P(None, "row"), P(None, "col"))

    def body(*args):
        return on_device(n, *args)

    return jax.shard_map(
        body,
        mesh=mesh,
        in_specs=placed,
        out_specs=(P(None, "row", "col"), P(None, "row"), P(None, "col")),
        check_vma=False,
    )
```
